32 devices in a mesh: seq: 8 (over z, x), res: 4 (over y, core).
Axes of the slice: x: 2, y: 2, z: 4, core: 2. Of those that a mesh axis runs over, the one named last changes fastest.
Arguments:
- alignment: bfloat16 [128, 256, 256], P('res', 'seq'), may hold values from -6 to 6
- alignment_mask: int32 [128, 256], P('res', 'seq'), may hold values from 0 to 1, as said below
- residue_mask: int32 [256], replicated, may hold values from 0 to 1, as said below
- pair_input: float32 [256, 256, 128], P('seq', 'res'), may hold values from -6 to 6
- outer_gain: float32 [256], replicated, may hold values from 0.25 to 1.75
- left_weight: bfloat16 [256, 32], replicated, may hold values from -0.375 to 0.375
- right_weight: bfloat16 [256, 32], replicated, may hold values from -0.375 to 0.375
- outer_weight: bfloat16 [1024, 128], replicated, may hold values from -1 to 1
- pair_gain: float32 [128], replicated, may hold values from 0.25 to 1.75
- bias_weight: bfloat16 [128, 8], replicated, may hold values from -48 to 48
- row_gain: float32 [256], replicated, may hold values from 0.25 to 1.75
- query_weight: bfloat16 [256, 256], replicated, may hold values from -0.375 to 0.375
- key_weight: bfloat16 [256, 256], replicated, may hold values from -0.375 to 0.375
- value_weight: bfloat16 [256, 256], replicated, may hold values from -0.375 to 0.375
- gate_weight: bfloat16 [256, 256], replicated, may hold values from -0.375 to 0.375
- output_weight: bfloat16 [256, 256], replicated, may hold values from -2 to 2
- transition_gain: float32 [256], replicated, may hold values from 0.25 to 1.75
- up_weight: bfloat16 [256, 1024], replicated, may hold values from -0.375 to 0.375
- down_weight: bfloat16 [1024, 256], replicated, may hold values from -0.1875 to 0.1875
Outputs:
- pair_output: float32 [256, 256, 128], P('seq', 'res')
- alignment_output: float32 [128, 256, 256], P('res', 'seq')
The draws below stay inside these ranges and needn't reach their ends.
Inputs may be any that keep to these rules, and one draw needn't show every extreme that they name: `residue_mask`: 1 for a present residue, 0 for padding; at least one residue is 1 and at least one is 0. Some residue whose residue_mask is 1 has alignment_mask 1 in every sequence.
All inputs are finite; a program needn't handle non-finite values.
Results may differ from the reference program's by a relative error of at most 0.04.
Values may be sent and summed in bfloat16 or wider, within the bound.
No kernel may reach another device: no remote copies, remote signals or barrier semaphores. Data moves between devices by JAX's collectives and lax.ppermute only.
A program may use at most 128 MiB of HBM per device.

```python
import math
import jax
import jax.numpy as jnp
from jax import lax

C_M = 256
C_Z = 128
HEADS = 8
HEAD = 32
OPM = 32
FF = 1024
SEQS = 128
RES = 256


def mask_draws(key):
    base_key = jax.random.fold_in(key, 7001)
    mask_key, row_key, anchor_key, gap_key = jax.random.split(base_key, 4)
    anchor = jax.random.randint(anchor_key, (), 0, RES)
    gap = (anchor + 1 + jax.random.randint(gap_key, (), 0, RES - 1)) % RES
    positions = jnp.arange(RES)
    residue_draw = (jax.random.randint(mask_key, (RES,), 0, 8) > 0).astype(jnp.int32)
    residue_draw = jnp.where(positions == gap, 0, residue_draw)
    residue_draw = jnp.where(positions == anchor, 1, residue_draw)
    alignment_draw = (jax.random.randint(row_key, (SEQS, RES), 0, 4) > 0).astype(jnp.int32)
    alignment_draw = jnp.where(positions[None, :] == anchor, 1, alignment_draw)
    return (residue_draw, alignment_draw)


def draw_residue_mask(key, part):
    return mask_draws(key)[0]


def draw_alignment_mask(key, part):
    return mask_draws(key)[1]


def draw_bias_weight(key, part):
    base_key = jax.random.fold_in(key, 7003)
    normal_key = jax.random.fold_in(base_key, 0)
    weight = jax.random.normal(normal_key, (C_Z, HEADS), jnp.float32) * C_Z ** (-0.5)
    return jnp.clip(weight, -48.0, 48.0).astype(jnp.bfloat16)


def level_of(key, shape, shards, low, largest):
    gain, own = 1.0, jax.random.fold_in(key, 6)
    for axis_at, shards_of in shards:
        heights = jnp.exp(jax.random.uniform(jax.random.fold_in(own, axis_at), (shards_of,), jnp.float32, low / len(shards), largest / len(shards)))
        gain = gain * jnp.repeat(heights, shape[axis_at] // shards_of).reshape([-1 if axis == axis_at else 1 for axis in range(len(shape))])
    return gain


def scatter_about(own_key, dims, scale, bound, pieces=(), kind=jnp.bfloat16):
    values = jax.random.normal(own_key, dims, jnp.float32) * scale
    if len(pieces) > 0:
        values = level_of(own_key, dims, pieces, -0.22, 0.18) * values
    return jnp.clip(values, min=-bound, max=bound).astype(kind)


def setup_inputs(seed: int = 0) -> dict:
    arg_keys = jax.random.split(jax.random.key(seed), 20)
    return {
        "alignment": scatter_about(arg_keys[0], (SEQS, RES, C_M), 1.0, 6.0, ((0, 4), (1, 8))),
        "alignment_mask": draw_alignment_mask(jax.random.fold_in(arg_keys[19], 71), 0),
        "residue_mask": draw_residue_mask(jax.random.fold_in(arg_keys[19], 71), 0),
        "pair_input": scatter_about(arg_keys[3], (RES, RES, C_Z), 1.0, 6.0, ((0, 8), (1, 4)), jnp.float32),
        "outer_gain": jnp.clip(1.0 + 0.15 * jax.random.normal(arg_keys[4], (C_M,), jnp.float32), 0.25, 1.75),
        "left_weight": scatter_about(arg_keys[5], (C_M, OPM), C_M ** -0.5, 0.375),
        "right_weight": scatter_about(arg_keys[6], (C_M, OPM), C_M ** -0.5, 0.375),
        "outer_weight": scatter_about(arg_keys[7], (OPM * OPM, C_Z), OPM ** -0.5, 1.0),
        "pair_gain": jnp.clip(1.0 + 0.15 * jax.random.normal(arg_keys[8], (C_Z,), jnp.float32), 0.25, 1.75),
        "bias_weight": draw_bias_weight(jax.random.fold_in(arg_keys[19], 71), 0),
        "row_gain": jnp.clip(1.0 + 0.15 * jax.random.normal(arg_keys[10], (C_M,), jnp.float32), 0.25, 1.75),
        "query_weight": scatter_about(arg_keys[11], (C_M, HEADS * HEAD), C_M ** -0.5, 0.375),
        "key_weight": scatter_about(arg_keys[12], (C_M, HEADS * HEAD), C_M ** -0.5, 0.375),
        "value_weight": scatter_about(arg_keys[13], (C_M, HEADS * HEAD), C_M ** -0.5, 0.375),
        "gate_weight": scatter_about(arg_keys[14], (C_M, HEADS * HEAD), C_M ** -0.5, 0.375),
        "output_weight": scatter_about(arg_keys[15], (HEADS * HEAD, C_M), (HEAD // 4) ** -0.5, 2.0),
        "transition_gain": jnp.clip(1.0 + 0.15 * jax.random.normal(arg_keys[16], (C_M,), jnp.float32), 0.25, 1.75),
        "up_weight": scatter_about(arg_keys[17], (C_M, FF), C_M ** -0.5, 0.375),
        "down_weight": scatter_about(arg_keys[18], (FF, C_M), FF ** -0.5, 0.1875),
    }


EPSILON = 1e-05
MASKED = -1000000000.0

def layer_norm(values, scales):
    values = values.astype(jnp.float32)
    center = values - lax.optimization_barrier(jnp.mean(values, -1, keepdims=True))
    spread = lax.optimization_barrier(jnp.mean(center * center, -1, keepdims=True))
    return center * lax.rsqrt(spread + EPSILON) * scales

def project(values, weight):
    flattened = values.reshape(-1, values.shape[-1])
    result = jnp.dot(flattened, weight, preferred_element_type=jnp.float32)
    return result.reshape(values.shape[:-1] + (weight.shape[1],))

def reference(alignment, alignment_mask, residue_mask, pair_input, outer_gain, left_weight, right_weight, outer_weight, pair_gain, bias_weight, row_gain, query_weight, key_weight, value_weight, gate_weight, output_weight, transition_gain, up_weight, down_weight):
    live_mask = (alignment_mask * residue_mask[None, :]).astype(jnp.float32)
    outer_norm = layer_norm(alignment, outer_gain).astype(jnp.bfloat16)
    left_proj = (project(outer_norm, left_weight) * live_mask[..., None]).astype(jnp.bfloat16)
    right_proj = (project(outer_norm, right_weight) * live_mask[..., None]).astype(jnp.bfloat16)
    row_block = math.gcd(RES, 16)

    def outer_rows(row_start):
        left_piece = lax.dynamic_slice_in_dim(left_proj, row_start, row_block, 1).astype(jnp.float32)
        product = jnp.einsum('sic,sje->ijce', left_piece, right_proj.astype(jnp.float32)).astype(jnp.bfloat16)
        update = jnp.dot(product.reshape(row_block * RES, OPM * OPM), outer_weight, preferred_element_type=jnp.float32).reshape(row_block, RES, C_Z)
        live_rows = lax.dynamic_slice_in_dim(live_mask, row_start, row_block, 1)
        counts = jnp.einsum('si,sj->ij', live_rows, live_mask)
        return update / jnp.maximum(counts, 1.0)[..., None]
    starts = jnp.arange(RES // row_block, dtype=jnp.int32) * row_block
    outer_update = lax.map(outer_rows, starts).reshape(RES, RES, C_Z)
    pair_output = pair_input + outer_update
    pair_norm = layer_norm(pair_output, pair_gain).astype(jnp.bfloat16)
    pair_bias = project(pair_norm, bias_weight).astype(jnp.bfloat16)
    head_bias = jnp.transpose(pair_bias, (2, 0, 1)).astype(jnp.float32)
    row_norm = layer_norm(alignment, row_gain).astype(jnp.bfloat16)
    query_proj = project(row_norm, query_weight).astype(jnp.bfloat16)
    key_proj = project(row_norm, key_weight).astype(jnp.bfloat16)
    value_proj = project(row_norm, value_weight).astype(jnp.bfloat16)
    gate_values = jax.nn.sigmoid(project(row_norm, gate_weight))
    score_scale = HEAD ** (-0.5)

    def attend(inputs):
        query_row, key_row, value_row, live_row = inputs
        query_heads = query_row.astype(jnp.float32).reshape(RES, HEADS, HEAD)
        key_heads = key_row.astype(jnp.float32).reshape(RES, HEADS, HEAD)
        value_heads = value_row.astype(jnp.float32).reshape(RES, HEADS, HEAD)
        scores = jnp.einsum('ihd,jhd->hij', query_heads, key_heads) * score_scale + head_bias
        scores = jnp.where(live_row[None, None, :] > 0, scores, MASKED)
        score_peaks = lax.optimization_barrier(jnp.max(scores, -1, keepdims=True))
        weights = jnp.exp(scores - score_peaks)
        totals = lax.optimization_barrier(jnp.sum(weights, -1))
        rounded = lax.optimization_barrier(weights.astype(jnp.bfloat16)).astype(jnp.float32)
        mixed_sum = jnp.einsum('hij,jhd->ihd', rounded, value_heads)
        return (mixed_sum / jnp.transpose(totals)[..., None]).reshape(RES, HEADS * HEAD)
    attended = lax.map(attend, (query_proj, key_proj, value_proj, live_mask))
    gated_rows = (attended * gate_values).astype(jnp.bfloat16)
    after_rows = alignment.astype(jnp.float32) + project(gated_rows, output_weight)
    trans_norm = layer_norm(after_rows, transition_gain).astype(jnp.bfloat16)
    hidden_units = jnp.maximum(project(trans_norm, up_weight), 0.0).astype(jnp.bfloat16)
    alignment_output = after_rows + project(hidden_units, down_weight)
    return (pair_output, alignment_output)
```

```python
import functools
import math

import jax
import jax.numpy as jnp
from jax import lax
from jax.experimental import pallas as pl
from jax.experimental.pallas import tpu as pltpu
from jax.sharding import PartitionSpec as P


EPSILON = 1e-05
MASKED = -1000000000.0
LANES = 128
ROW_STEP = 256
PACK = 8
VMEM_BYTES = 40 * 1024 * 1024
ALL_VMEM_BYTES = 60 * 1024 * 1024
F32 = jnp.float32
BF16 = jnp.bfloat16


def normalized(values, gain):
    center = values - jnp.mean(values, -1, keepdims=True)
    spread = jnp.mean(center * center, -1, keepdims=True)
    return center * lax.rsqrt(spread + EPSILON) * gain


def dot(left, right, dims=((1,), (0,))):
    return lax.dot_general(left, right, (dims, ((), ())), preferred_element_type=F32)


def where_matrix(shape, test):
    rows = lax.broadcasted_iota(jnp.int32, shape, 0)
    lanes = lax.broadcasted_iota(jnp.int32, shape, 1)
    return jnp.where(test(rows, lanes), 1.0, 0.0).astype(BF16)


def swapped(arrays, axis):
    size = lax.axis_size(axis)
    assert size & (size - 1) == 0
    come = []
    for k, array in enumerate(arrays):
        pairs = [(i, i ^ k) for i in range(size)]
        come.append(lax.ppermute(array, axis, pairs) if k else array)
    return come


def whole(shape):
    return pl.BlockSpec(shape, lambda *_: (0,) * len(shape))


def params(limit=VMEM_BYTES):
    return pltpu.CompilerParams(vmem_limit_bytes=limit)


def factor_kernel(
    sizes,
    x_ref,
    mask_ref,
    residue_ref,
    gain_ref,
    left_w_ref,
    right_w_ref,
    left_ref,
    right_ref,
    norm_ref,
    rows_ref,
):
    seqs, residues, width = sizes
    norm = normalized(x_ref[...].astype(F32), gain_ref[...])
    groups = residues // PACK
    for part in range(norm_ref.shape[0]):
        lanes = slice(part * LANES, (part + 1) * LANES)
        norm_ref[part] = norm[:, lanes]
        for place in range(PACK):
            for group in range(groups):
                at = (place * groups + group) * seqs
                rows_ref[at : at + seqs, lanes] = norm_ref[
                    part, pl.ds(group * PACK + place, seqs, stride=residues), :
                ].astype(BF16)
    span = PACK * width
    spread_left = where_matrix((width, span), lambda r, l: r == l % width)
    spread_right = where_matrix((width, span), lambda r, l: r == l // PACK)
    left_wide = dot(left_w_ref[...], spread_left, ((0,), (0,))).astype(BF16)
    right_wide = dot(right_w_ref[...], spread_right, ((0,), (0,))).astype(BF16)
    rows = rows_ref[...]
    start = lax.axis_index("seq") * residues
    own = where_matrix((residue_ref.shape[1], residues), lambda r, l: r == l + start)
    row_live = dot(residue_ref[...].astype(F32).astype(BF16), own)
    live = (mask_ref[...].astype(F32) * row_live).astype(BF16)
    total = residues * width
    live_left = dot(live, where_matrix((residues, total), lambda r, l: r == l // width))
    live_right = dot(
        live,
        where_matrix((residues, total), lambda r, l: r == (l // span) * PACK + l % PACK),
    )
    live_plain = dot(live, where_matrix((residues, LANES), lambda r, l: r == l)).astype(BF16)
    lane = lax.broadcasted_iota(jnp.int32, (groups * seqs, span), 1)
    for wide, out_refs, live_wide, place_of in (
        (left_wide, [left_ref], live_left, lane // width),
        (
            right_wide,
            [right_ref.at[copy] for copy in range(right_ref.shape[0])],
            live_right,
            lane % PACK,
        ),
    ):
        product = dot(rows, wide)
        packed = product[: groups * seqs]
        for place in range(1, PACK):
            packed = jnp.where(
                place_of == place,
                product[place * groups * seqs : (place + 1) * groups * seqs],
                packed,
            )
        pieces = []
        for group in range(groups):
            piece = packed[group * seqs : (group + 1) * seqs]
            pieces.append((piece * live_wide[:, group * span : (group + 1) * span]).astype(BF16))
        for out_ref in out_refs:
            for group in range(groups):
                out_ref[:, group * span : (group + 1) * span] = pieces[group]
            out_ref[:, total:] = live_plain


def project_kernel(sizes, x_ref, gain_ref, qw_ref, kw_ref, vw_ref, gw_ref, *refs):
    seqs, residues, heads, head, shares, query_scale = sizes
    *sent_refs, gate_ref, rows_ref, qkv_ref = refs
    pack = LANES // head
    groups = seqs // pack
    block = groups * residues
    norm = normalized(x_ref[...].astype(F32), gain_ref[...]).astype(BF16)
    for seq in range(seqs):
        at = (seq % pack) * block + (seq // pack) * residues
        rows_ref[at : at + residues, :] = norm[seq * residues : (seq + 1) * residues]
    features = heads * head
    pair = 2 * LANES
    lane = lax.broadcasted_iota(jnp.int32, (block, pair), 1)
    place_of = (lane % LANES) // head
    own = groups // shares
    for kind, w_ref in enumerate((qw_ref, kw_ref, vw_ref, gw_ref)):
        for two in range(heads // 2):
            base = two * 2 * head
            spread = where_matrix(
                (features, pair),
                lambda r, l: r == base + (l // LANES) * head + l % head,
            )
            wide = dot(w_ref[...], spread).astype(BF16)
            product = dot(rows_ref[...], wide)
            packed = product[:block]
            for place in range(1, pack):
                packed = jnp.where(
                    place_of == place, product[place * block : (place + 1) * block], packed
                )
            if kind == 0:
                packed = packed * query_scale
            if kind == 3:
                packed = jax.nn.sigmoid(packed)
            else:
                packed = packed.astype(BF16)
            for one in range(2):
                for group in range(groups):
                    piece = packed[
                        group * residues : (group + 1) * residues, one * LANES : (one + 1) * LANES
                    ]
                    to = (two * 2 + one) * shares + group // own
                    lanes = slice((group % own) * LANES, (group % own + 1) * LANES)
                    if kind == 3:
                        gate_ref[to, :, lanes] = piece
                    else:
                        qkv_ref[to, kind, :, lanes] = piece
    me = lax.axis_index("seq")
    for offset, sent_ref in enumerate(sent_refs):
        sent_ref[...] = qkv_ref[me ^ offset]


def mask_kernel(sizes, rows_ref, out_ref):
    residues, shares = sizes
    blocks, seqs, _ = rows_ref.shape
    groups, pack, length = out_ref.shape
    live = jnp.zeros((seqs, length), F32)
    for block in range(blocks):
        place = where_matrix((LANES, length), lambda r, l: l == r + block * residues)
        inside = lax.broadcasted_iota(jnp.int32, (LANES, length), 0) < residues
        live = live + dot(rows_ref[block], jnp.where(inside, place, jnp.zeros_like(place)))
    if shares > 1:
        first = (lax.axis_index("seq") % shares) * groups * pack
        chosen = where_matrix((groups * pack, seqs), lambda r, l: l == r + first)
        live = dot(chosen, live.astype(BF16))
    added = (1.0 - live) * MASKED
    for group in range(groups):
        out_ref[group] = added[group * pack : (group + 1) * pack]


def weight_kernel(sizes, outer_w_ref, blocks_ref):
    width, pair_width = sizes
    quad = LANES // width
    blocks_ref[...] = jnp.zeros_like(blocks_ref)
    for e in range(width):
        piece = outer_w_ref[e * width : (e + 1) * width, :]
        for place in range(quad):
            row = e * LANES + place * width
            blocks_ref[row : row + width, place * pair_width : (place + 1) * pair_width] = piece


def widen_kernel(sizes, out_w_ref, wide_ref):
    heads, head = sizes
    spread = where_matrix(
        (heads * LANES, heads * head), lambda r, l: (r // LANES) * head + r % head == l
    )
    wide_ref[...] = dot(spread, out_w_ref[...]).astype(BF16)


def outer_kernel(sizes, right_ref, pair_ref, weight_ref, gain_ref, bias_w_ref, *refs):
    residues, columns, width, pair_width, seqs, shares = sizes
    members = right_ref.shape[0]
    left_refs = refs[:members]
    out_ref, bias_ref, left_ref, stage_ref, norm_ref, bias_rows_ref = refs[members : members + 6]
    held_ref, held_pair_ref, weight_sem, pair_sem = refs[members + 6 :]
    weight_copy = pltpu.make_async_copy(weight_ref, held_ref, weight_sem)
    weight_copy.start()
    pair_copy = pltpu.make_async_copy(pair_ref, held_pair_ref, pair_sem)
    pair_copy.start()
    share = seqs // members
    me = lax.axis_index("res")
    for offset, member_ref in enumerate(left_refs):
        at = pl.multiple_of((me ^ offset) * share, share)
        left_ref[pl.ds(at, share), :] = member_ref[...]
    span = PACK * width
    quad = LANES // width
    groups = residues // quad
    total = residues * width
    blocks = right_ref.shape[1]
    live_left = left_ref[:, total : total + LANES]
    counts = []
    for block in range(blocks):
        live_right = right_ref[:, block, :, total : total + LANES].reshape(seqs, LANES)
        counts.append(dot(live_right.T, live_left)[:residues])
        for two in range(residues // (2 * PACK)):
            flipped = []
            for one in range(2):
                lanes = slice((two * 2 + one) * span, (two * 2 + one + 1) * span)
                flipped.append(right_ref[:, block, :, lanes].reshape(seqs, span).T)
            row = block * residues + two * 2 * PACK
            for chunk in range(total // (2 * LANES)):
                left = left_ref[:, chunk * 2 * LANES : (chunk + 1) * 2 * LANES]
                products = [
                    dot(member, left).reshape(width, PACK, 2 * LANES) for member in flipped
                ]
                joined = jnp.concatenate(products, axis=1).astype(BF16)
                for one in range(2):
                    at = (chunk * 2 + one) * columns + row
                    for e in range(width):
                        stage_ref[at : at + 2 * PACK, e * LANES : (e + 1) * LANES] = joined[
                            e, :, one * LANES : (one + 1) * LANES
                        ]
    scale = 1.0 / jnp.maximum(jnp.concatenate(counts, axis=0), 1.0)
    gain = gain_ref[...]
    weight_copy.wait()
    pair_copy.wait()
    for two in range(quad // 2):
        lanes = slice(two * 2 * pair_width, (two + 1) * 2 * pair_width)
        update = dot(stage_ref[...], held_ref[:, lanes])
        for group in range(groups):
            for one in range(2):
                i = group * quad + two * 2 + one
                piece = update[
                    group * columns : (group + 1) * columns,
                    one * pair_width : (one + 1) * pair_width,
                ]
                value = held_pair_ref[i] + piece * scale[:, i : i + 1]
                out_ref[i] = value
                norm_ref[i] = normalized(value, gain).astype(BF16)
    halves = LANES // columns
    rows = residues // halves
    for row in range(rows):
        joined = jnp.concatenate([norm_ref[row + half * rows] for half in range(halves)], axis=0)
        bias = dot(bias_w_ref[...], joined, ((1,), (1,)))
        for head in range(bias_w_ref.shape[0]):
            bias_rows_ref[head, row : row + 1, :] = bias[head : head + 1, :]
    for to in range(bias_ref.shape[0]):
        piece = bias_rows_ref[to // shares].astype(BF16)
        for other in range(bias_ref.shape[1]):
            bias_ref[to, other] = piece


def attention_kernel(sizes, bias_ref, mask_ref, *refs):
    residues, columns, head, row_step = sizes
    *come_refs, out_ref, full_ref, qkv_ref = refs
    blocks = len(come_refs)
    length = blocks * residues
    me = lax.axis_index("seq")
    for offset, come_ref in enumerate(come_refs):
        at = pl.multiple_of((me ^ offset) * residues, residues)
        for kind in range(3):
            qkv_ref[kind, pl.ds(at, residues), :] = come_ref[kind]
    others = bias_ref.shape[1]
    halves = LANES // columns
    rows = residues // halves

    @pl.when(pl.program_id(0) == 0)
    def _():
        pieces = jnp.concatenate(
            [bias_ref[:, other].reshape(blocks * rows, LANES) for other in range(others)], axis=1
        )
        for half in range(halves):
            place = where_matrix(
                (others * LANES, length),
                lambda r, l: ((r // columns) % halves == half)
                & ((r // LANES) * columns + r % columns == l),
            )
            placed = dot(pieces, place) * math.log2(math.e)
            for block in range(blocks):
                at = block * residues + half * rows
                full_ref[at : at + rows, :] = placed[block * rows : (block + 1) * rows]

    pack = LANES // head
    keys = qkv_ref[1]
    values = qkv_ref[2]
    lane = lax.broadcasted_iota(jnp.int32, (length, LANES), 1) // head
    zeros = jnp.zeros_like(keys)
    ones = jnp.ones_like(keys)
    key_of = [jnp.where(lane == place, keys, zeros) for place in range(pack)]
    value_of = [
        jnp.concatenate(
            [jnp.where(lane == place, values, zeros), jnp.where(lane == place, ones, zeros)], axis=1
        )
        for place in range(pack)
    ]
    value_all = jnp.concatenate(value_of, axis=0)
    per = row_step // residues
    for step in range(length // row_step):
        rows = slice(step * row_step, (step + 1) * row_step)
        queries = qkv_ref[0, rows, :]
        bias = full_ref[rows, :]
        weights = []
        for place in range(pack):
            scores = dot(queries, key_of[place], ((1,), (1,))) + bias + mask_ref[0, place : place + 1]
            weights.append(jnp.exp2(scores - jnp.max(scores, -1, keepdims=True)).astype(BF16))
        both = dot(jnp.concatenate(weights, axis=1), value_all)
        out_ref[step * per : (step + 1) * per] = (
            (both[:, :LANES] / both[:, LANES:]).astype(BF16).reshape(per, residues, LANES)
        )


def finish_kernel(
    sizes, mixed_ref, gate_ref, x_ref, wide_ref, gain_ref, up_ref, down_ref, out_ref
):
    residues, heads, head, _, groups = sizes
    pack = LANES // head
    gated = []
    for group in range(groups):
        lanes = slice(group * LANES, (group + 1) * LANES)
        gated.append(
            jnp.concatenate(
                [
                    (mixed_ref[h, :, lanes].astype(F32) * gate_ref[h, :, lanes]).astype(BF16)
                    for h in range(heads)
                ],
                axis=1,
            )
        )
    gated = jnp.concatenate(gated, axis=0)
    lane = lax.broadcasted_iota(jnp.int32, gated.shape, 1)
    place_of = (lane % LANES) // head
    chosen = jnp.concatenate(
        [jnp.where(place_of == place, gated, jnp.zeros_like(gated)) for place in range(pack)], axis=0
    )
    added = dot(chosen, wide_ref[...])
    order = [group * pack + place for place in range(pack) for group in range(groups)]
    x = jnp.concatenate([x_ref[seq] for seq in order], axis=0).astype(F32)
    after = x + added
    norm = normalized(after, gain_ref[...]).astype(BF16)
    hidden = jnp.maximum(dot(norm, up_ref[...]), 0.0).astype(BF16)
    result = after + dot(hidden, down_ref[...])
    for at, seq in enumerate(order):
        out_ref[seq] = result[at * residues : (at + 1) * residues]


def on_device(
    alignment,
    alignment_mask,
    residue_mask,
    pair_input,
    outer_gain,
    left_weight,
    right_weight,
    outer_weight,
    pair_gain,
    bias_weight,
    row_gain,
    query_weight,
    key_weight,
    value_weight,
    gate_weight,
    output_weight,
    transition_gain,
    up_weight,
    down_weight,
):
    seqs, residues, channels = alignment.shape
    columns, pair_width = pair_input.shape[1:]
    seq_axis, res_axis = lax.axis_size("seq"), lax.axis_size("res")
    heads = bias_weight.shape[1]
    head = query_weight.shape[1] // heads
    width = left_weight.shape[1]
    all_seqs, length = seqs * res_axis, residues * seq_axis
    shares = seq_axis // heads
    own = seqs // shares
    pack = LANES // head
    assert shares * heads == seq_axis and own % pack == 0
    blocks = seq_axis // res_axis
    assert blocks * residues == columns

    flat = alignment.reshape(seqs * residues, channels)
    wide = residues * width + LANES

    left, right = pl.pallas_call(
        functools.partial(factor_kernel, (seqs, residues, width)),
        out_shape=(
            jax.ShapeDtypeStruct((seqs, wide), BF16),
            jax.ShapeDtypeStruct((seq_axis, seqs, wide), BF16),
        ),
        scratch_shapes=[
            pltpu.VMEM((channels // LANES, seqs * residues, LANES), F32),
            pltpu.VMEM((seqs * residues, channels), BF16),
        ],
        compiler_params=params(ALL_VMEM_BYTES),
        cost_estimate=pl.CostEstimate(
            flops=2 * seqs * residues * channels * 2 * PACK * width, bytes_accessed=1 << 20,
            transcendentals=0,
        ),
        name="factors",
    )(flat, alignment_mask, residue_mask[None], outer_gain[None], left_weight.T, right_weight.T)

    right_rows = lax.all_to_all(right, "seq", split_axis=0, concat_axis=0, tiled=True)
    left_all = swapped([left] * res_axis, "res")

    *qkv, gates = pl.pallas_call(
        functools.partial(
            project_kernel,
            (seqs, residues, heads, head, shares, head ** (-0.5) * math.log2(math.e)),
        ),
        out_shape=(
            *(jax.ShapeDtypeStruct((3, residues, own * head), BF16),) * seq_axis,
            jax.ShapeDtypeStruct((seq_axis, residues, own * head), F32),
        ),
        scratch_shapes=[
            pltpu.VMEM((seqs * residues, channels), BF16),
            pltpu.VMEM((seq_axis, 3, residues, own * head), BF16),
        ],
        compiler_params=params(ALL_VMEM_BYTES),
        cost_estimate=pl.CostEstimate(
            flops=2 * seqs * residues * channels * 4 * heads * LANES, bytes_accessed=4 << 20,
            transcendentals=seqs * residues * channels,
        ),
        name="projections",
    )(flat, row_gain[None], query_weight, key_weight, value_weight, gate_weight)

    right_all = lax.all_to_all(right_rows, "res", split_axis=0, concat_axis=0, tiled=True)
    qkv_all = swapped(qkv, "seq")

    mask = pl.pallas_call(
        functools.partial(mask_kernel, (residues, shares)),
        grid=(1,),
        in_specs=[
            pl.BlockSpec((seq_axis, seqs, LANES), lambda _: (0, 0, residues * width // LANES))
        ],
        out_specs=whole((own // pack, pack, length)),
        out_shape=jax.ShapeDtypeStruct((own // pack, pack, length), F32),
        compiler_params=params(),
        cost_estimate=pl.CostEstimate(flops=1 << 26, bytes_accessed=1 << 17, transcendentals=0),
        name="mask",
    )(right_rows)

    flipped_w = outer_weight.reshape(width, width, pair_width).swapaxes(0, 1)
    flipped_w = flipped_w.reshape(width * width, pair_width)
    quad = LANES // width
    wide_outer = pl.pallas_call(
        functools.partial(weight_kernel, (width, pair_width)),
        out_shape=jax.ShapeDtypeStruct((width * LANES, quad * pair_width), BF16),
        compiler_params=params(ALL_VMEM_BYTES),
        cost_estimate=pl.CostEstimate(flops=1 << 29, bytes_accessed=5 << 20, transcendentals=0),
        name="weights",
    )(flipped_w)
    wide_output = pl.pallas_call(
        functools.partial(widen_kernel, (heads, head)),
        out_shape=jax.ShapeDtypeStruct((heads * LANES, channels), BF16),
        compiler_params=params(ALL_VMEM_BYTES),
        cost_estimate=pl.CostEstimate(flops=1 << 28, bytes_accessed=1 << 19, transcendentals=0),
        name="widen",
    )(output_weight)
    halves = LANES // columns
    bias_rows = residues // halves
    pair_output, bias = pl.pallas_call(
        functools.partial(
            outer_kernel, (residues, columns, width, pair_width, all_seqs, shares)
        ),
        in_specs=[
            pl.BlockSpec(memory_space=pl.ANY if at in (1, 2) else pltpu.VMEM)
            for at in range(5 + res_axis)
        ],
        out_shape=(
            jax.ShapeDtypeStruct(pair_input.shape, F32),
            jax.ShapeDtypeStruct((seq_axis, res_axis, bias_rows, LANES), BF16),
        ),
        scratch_shapes=[
            pltpu.VMEM((all_seqs, wide), BF16),
            pltpu.VMEM((residues // quad * columns, width * LANES), BF16),
            pltpu.VMEM((residues, columns, pair_width), BF16),
            pltpu.VMEM((heads, bias_rows, LANES), F32),
            pltpu.VMEM((width * LANES, quad * pair_width), BF16),
            pltpu.VMEM(pair_input.shape, F32),
            pltpu.SemaphoreType.DMA,
            pltpu.SemaphoreType.DMA,
        ],
        compiler_params=params(ALL_VMEM_BYTES),
        cost_estimate=pl.CostEstimate(
            flops=2 * residues * columns * width * width * (all_seqs + 4 * pair_width),
            bytes_accessed=4 << 20,
            transcendentals=0,
        ),
        name="outer",
    )(
        right_all.reshape(res_axis, blocks, seqs, wide),
        pair_input,
        wide_outer,
        pair_gain[None],
        bias_weight.T,
        *left_all,
    )
    bias_all = lax.all_to_all(
        bias.reshape(seq_axis * res_axis, bias_rows, LANES),
        ("seq", "res"),
        split_axis=0,
        concat_axis=0,
        tiled=True,
    ).reshape(seq_axis, res_axis, bias_rows, LANES)

    mixed = pl.pallas_call(
        functools.partial(
            attention_kernel, (residues, columns, head, max(residues, min(length, ROW_STEP)))
        ),
        grid=(own // pack,),
        in_specs=[
            whole((seq_axis, res_axis, bias_rows, LANES)),
            pl.BlockSpec((1, pack, length), lambda g: (g, 0, 0)),
            *(pl.BlockSpec((3, residues, LANES), lambda g: (0, 0, g)),) * seq_axis,
        ],
        out_specs=pl.BlockSpec((seq_axis, residues, LANES), lambda g: (0, 0, g)),
        out_shape=jax.ShapeDtypeStruct((seq_axis, residues, own * head), BF16),
        scratch_shapes=[
            pltpu.VMEM((length, length), F32),
            pltpu.VMEM((3, length, LANES), BF16),
        ],
        compiler_params=params(),
        cost_estimate=pl.CostEstimate(
            flops=4 * own * length * length * LANES, bytes_accessed=2 << 20,
            transcendentals=own * length * length,
        ),
        name="attention",
    )(bias_all, mask, *qkv_all)

    mixed_home = lax.all_to_all(mixed, "seq", split_axis=0, concat_axis=0, tiled=True)

    steps = 2 * shares
    groups = seqs // pack // steps
    per_share = own // pack // groups
    if shares > 1:
        mixed_home = mixed_home.reshape(heads, shares, residues, own * head)
        gates = gates.reshape(heads, shares, residues, own * head)
        share_spec = pl.BlockSpec(
            (heads, None, residues, groups * LANES), lambda g: (0, g // per_share, 0, g % per_share)
        )
    else:
        share_spec = pl.BlockSpec((heads, residues, groups * LANES), lambda g: (0, 0, g))
    hidden = up_weight.shape[1]
    alignment_output = pl.pallas_call(
        functools.partial(finish_kernel, (residues, heads, head, shares, groups)),
        grid=(steps,),
        in_specs=[
            share_spec,
            share_spec,
            pl.BlockSpec((groups * pack, residues, channels), lambda g: (g, 0, 0)),
            whole((heads * LANES, channels)),
            whole((1, channels)),
            whole(up_weight.shape),
            whole(down_weight.shape),
        ],
        out_specs=pl.BlockSpec((groups * pack, residues, channels), lambda g: (g, 0, 0)),
        out_shape=jax.ShapeDtypeStruct(alignment.shape, F32),
        compiler_params=params(),
        cost_estimate=pl.CostEstimate(
            flops=2 * seqs * residues * channels * (4 * channels + 2 * hidden),
            bytes_accessed=4 << 20,
            transcendentals=0,
        ),
        name="finish",
    )(mixed_home, gates, alignment, wide_output, transition_gain[None], up_weight, down_weight)
    return (pair_output, alignment_output)


def solution(mesh):
    spread = P("res", "seq", None)
    pair = P("seq", "res", None)
    in_specs = (spread, P("res", "seq"), P(), pair) + (P(),) * 15

    return jax.shard_map(
        on_device, mesh=mesh, in_specs=in_specs, out_specs=(pair, spread), check_vma=False
    )
```

```python
import functools
import math

import jax
import jax.numpy as jnp
from jax import lax
from jax.experimental import pallas as pl
from jax.experimental.pallas import tpu as pltpu
from jax.sharding import PartitionSpec as P


EPSILON = 1e-05
MASKED = -1000000000.0
LANES = 128
ROW_STEP = 256
PACK = 8
VMEM_BYTES = 40 * 1024 * 1024
ALL_VMEM_BYTES = 60 * 1024 * 1024
F32 = jnp.float32
BF16 = jnp.bfloat16


def normalized(values, gain):
    center = values - jnp.mean(values, -1, keepdims=True)
    spread = jnp.mean(center * center, -1, keepdims=True)
    return center * lax.rsqrt(spread + EPSILON) * gain


def dot(left, right, dims=((1,), (0,))):
    return lax.dot_general(left, right, (dims, ((), ())), preferred_element_type=F32)


def where_matrix(shape, test):
    rows = lax.broadcasted_iota(jnp.int32, shape, 0)
    lanes = lax.broadcasted_iota(jnp.int32, shape, 1)
    return jnp.where(test(rows, lanes), 1.0, 0.0).astype(BF16)


def swapped(arrays, axis):
    size = lax.axis_size(axis)
    assert len(arrays) & (len(arrays) - 1) == 0 and size % len(arrays) == 0
    come = []
    for k, array in enumerate(arrays):
        pairs = [(i, i ^ k) for i in range(size)]
        come.append(lax.ppermute(array, axis, pairs) if k else array)
    return come


def whole(shape):
    return pl.BlockSpec(shape, lambda *_: (0,) * len(shape))


def params(limit=VMEM_BYTES):
    return pltpu.CompilerParams(vmem_limit_bytes=limit)


def factor_kernel(
    sizes,
    x_ref,
    mask_ref,
    residue_ref,
    gain_ref,
    left_w_ref,
    right_w_ref,
    left_ref,
    right_ref,
    norm_ref,
    rows_ref,
):
    seqs, residues, width = sizes
    norm = normalized(x_ref[...].astype(F32), gain_ref[...])
    groups = residues // PACK
    for part in range(norm_ref.shape[0]):
        lanes = slice(part * LANES, (part + 1) * LANES)
        norm_ref[part] = norm[:, lanes]
        for place in range(PACK):
            for group in range(groups):
                at = (place * groups + group) * seqs
                rows_ref[at : at + seqs, lanes] = norm_ref[
                    part, pl.ds(group * PACK + place, seqs, stride=residues), :
                ].astype(BF16)
    span = PACK * width
    spread_left = where_matrix((width, span), lambda r, l: r == l % width)
    spread_right = where_matrix((width, span), lambda r, l: r == l // PACK)
    left_wide = dot(left_w_ref[...], spread_left, ((0,), (0,))).astype(BF16)
    right_wide = dot(right_w_ref[...], spread_right, ((0,), (0,))).astype(BF16)
    rows = rows_ref[...]
    start = lax.axis_index("seq") * residues
    own = where_matrix((residue_ref.shape[1], residues), lambda r, l: r == l + start)
    row_live = dot(residue_ref[...].astype(F32).astype(BF16), own)
    live = (mask_ref[...].astype(F32) * row_live).astype(BF16)
    total = residues * width
    live_left = dot(live, where_matrix((residues, total), lambda r, l: r == l // width))
    live_right = dot(
        live,
        where_matrix((residues, total), lambda r, l: r == (l // span) * PACK + l % PACK),
    )
    live_plain = dot(live, where_matrix((residues, LANES), lambda r, l: r == l)).astype(BF16)
    lane = lax.broadcasted_iota(jnp.int32, (groups * seqs, span), 1)
    for wide, out_ref, live_wide, place_of in (
        (left_wide, left_ref, live_left, lane // width),
        (right_wide, right_ref, live_right, lane % PACK),
    ):
        product = dot(rows, wide)
        packed = product[: groups * seqs]
        for place in range(1, PACK):
            packed = jnp.where(
                place_of == place,
                product[place * groups * seqs : (place + 1) * groups * seqs],
                packed,
            )
        pieces = []
        for group in range(groups):
            piece = packed[group * seqs : (group + 1) * seqs]
            pieces.append((piece * live_wide[:, group * span : (group + 1) * span]).astype(BF16))
        for group in range(groups):
            out_ref[:, group * span : (group + 1) * span] = pieces[group]
        out_ref[:, total:] = live_plain


def project_heads(sizes, x_ref, gain_ref, rows_ref, w_refs, write):
    seqs, residues, heads, head, shares = sizes
    pack = LANES // head
    groups = seqs // pack
    block = groups * residues
    norm = normalized(x_ref[...].astype(F32), gain_ref[...]).astype(BF16)
    for seq in range(seqs):
        at = (seq % pack) * block + (seq // pack) * residues
        rows_ref[at : at + residues, :] = norm[seq * residues : (seq + 1) * residues]
    pair = 2 * LANES
    place_of = (lax.broadcasted_iota(jnp.int32, (block, pair), 1) % LANES) // head
    own = groups // shares
    for kind, w_ref in enumerate(w_refs):
        for two in range(heads // 2):
            base = two * 2 * head
            spread = where_matrix(
                (heads * head, pair), lambda r, l: r == base + (l // LANES) * head + l % head
            )
            product = dot(rows_ref[...], dot(w_ref[...], spread).astype(BF16))
            packed = product[:block]
            for place in range(1, pack):
                packed = jnp.where(
                    place_of == place, product[place * block : (place + 1) * block], packed
                )
            for one in range(2):
                done = packed[:, one * LANES : (one + 1) * LANES]
                for group in range(groups):
                    to = (two * 2 + one) * shares + group // own
                    lanes = slice((group % own) * LANES, (group % own + 1) * LANES)
                    write(kind, to, lanes, done[group * residues : (group + 1) * residues])


def gate_kernel(sizes, x_ref, gain_ref, w_ref, gate_ref, rows_ref):
    def write(kind, to, lanes, piece):
        gate_ref[to, :, lanes] = jax.nn.sigmoid(piece)

    project_heads(sizes, x_ref, gain_ref, rows_ref, [w_ref], write)


def project_kernel(sizes, scale, x_ref, gain_ref, qw_ref, kw_ref, vw_ref, *refs):
    *sent_refs, rows_ref, qkv_ref = refs

    def write(kind, to, lanes, piece):
        qkv_ref[to, kind, :, lanes] = (piece * scale if kind == 0 else piece).astype(BF16)

    project_heads(sizes, x_ref, gain_ref, rows_ref, [qw_ref, kw_ref, vw_ref], write)
    me = lax.axis_index("seq")
    for offset, sent_ref in enumerate(sent_refs):
        sent_ref[...] = qkv_ref[me ^ offset]


def assemble_kernel(*refs):
    *part_refs, out_ref = refs
    me = lax.axis_index("seq")
    for offset, part_ref in enumerate(part_refs):
        out_ref[me ^ offset] = part_ref[...]


def mask_kernel(sizes, rows_ref, out_ref):
    residues, shares = sizes
    blocks, seqs, _ = rows_ref.shape
    groups, pack, length = out_ref.shape
    live = jnp.zeros((seqs, length), F32)
    for block in range(blocks):
        place = where_matrix((LANES, length), lambda r, l: l == r + block * residues)
        inside = lax.broadcasted_iota(jnp.int32, (LANES, length), 0) < residues
        live = live + dot(rows_ref[block], jnp.where(inside, place, jnp.zeros_like(place)))
    if shares > 1:
        first = (lax.axis_index("seq") % shares) * groups * pack
        chosen = where_matrix((groups * pack, seqs), lambda r, l: l == r + first)
        live = dot(chosen, live.astype(BF16))
    added = (1.0 - live) * MASKED
    for group in range(groups):
        out_ref[group] = added[group * pack : (group + 1) * pack]


def widen_kernel(sizes, out_w_ref, wide_ref):
    heads, head = sizes
    spread = where_matrix(
        (heads * LANES, heads * head), lambda r, l: (r // LANES) * head + r % head == l
    )
    wide_ref[...] = dot(spread, out_w_ref[...]).astype(BF16)


def outer_kernel(sizes, right_ref, pair_ref, weight_ref, gain_ref, bias_w_ref, *refs):
    residues, columns, width, pair_width, seqs, shares = sizes
    members = right_ref.shape[0]
    left_refs = refs[:members]
    out_ref, bias_ref, left_ref, stage_ref, norm_ref, bias_rows_ref = refs[members : members + 6]
    held_ref, plain_ref, held_pair_ref, pair_sem = refs[members + 6 :]
    pair_copy = pltpu.make_async_copy(pair_ref, held_pair_ref, pair_sem)
    pair_copy.start()
    quad = LANES // width
    plain_ref[...] = weight_ref[...].astype(F32)
    held_ref[...] = jnp.zeros_like(held_ref)
    for e in range(width):
        piece = plain_ref[pl.ds(e, width, stride=width), :].astype(BF16)
        for place in range(quad):
            row = e * LANES + place * width
            held_ref[row : row + width, place * pair_width : (place + 1) * pair_width] = piece
    share = seqs // members
    me = lax.axis_index("res")
    for offset, member_ref in enumerate(left_refs):
        at = pl.multiple_of((me ^ offset) * share, share)
        left_ref[pl.ds(at, share), :] = member_ref[...]
    span = PACK * width
    groups = residues // quad
    total = residues * width
    blocks = right_ref.shape[1]
    live_left = left_ref[:, total : total + LANES]
    counts = []
    for block in range(blocks):
        live_right = right_ref[:, block, :, total : total + LANES].reshape(seqs, LANES)
        counts.append(dot(live_right.T, live_left)[:residues])
        for two in range(residues // (2 * PACK)):
            flipped = []
            for one in range(2):
                lanes = slice((two * 2 + one) * span, (two * 2 + one + 1) * span)
                flipped.append(right_ref[:, block, :, lanes].reshape(seqs, span).T)
            row = block * residues + two * 2 * PACK
            for chunk in range(total // (2 * LANES)):
                left = left_ref[:, chunk * 2 * LANES : (chunk + 1) * 2 * LANES]
                products = [
                    dot(member, left).reshape(width, PACK, 2 * LANES) for member in flipped
                ]
                joined = jnp.concatenate(products, axis=1).astype(BF16)
                for one in range(2):
                    at = (chunk * 2 + one) * columns + row
                    for e in range(width):
                        stage_ref[at : at + 2 * PACK, e * LANES : (e + 1) * LANES] = joined[
                            e, :, one * LANES : (one + 1) * LANES
                        ]
    scale = 1.0 / jnp.maximum(jnp.concatenate(counts, axis=0), 1.0)
    gain = gain_ref[...]
    pair_copy.wait()
    for two in range(quad // 2):
        lanes = slice(two * 2 * pair_width, (two + 1) * 2 * pair_width)
        update = dot(stage_ref[...], held_ref[:, lanes])
        for group in range(groups):
            for one in range(2):
                i = group * quad + two * 2 + one
                piece = update[
                    group * columns : (group + 1) * columns,
                    one * pair_width : (one + 1) * pair_width,
                ]
                value = held_pair_ref[i] + piece * scale[:, i : i + 1]
                out_ref[i] = value
                norm_ref[i] = normalized(value, gain).astype(BF16)
    halves = LANES // columns
    rows = residues // halves
    for row in range(rows):
        joined = jnp.concatenate([norm_ref[row + half * rows] for half in range(halves)], axis=0)
        bias = dot(bias_w_ref[...], joined, ((1,), (1,)))
        for head in range(bias_w_ref.shape[0]):
            bias_rows_ref[head, row : row + 1, :] = bias[head : head + 1, :]
    for to in range(bias_ref.shape[0]):
        piece = bias_rows_ref[to // shares].astype(BF16)
        for other in range(bias_ref.shape[1]):
            bias_ref[to, other] = piece


def attention_kernel(sizes, bias_ref, mask_ref, *refs):
    residues, columns, head, row_step = sizes
    *come_refs, out_ref, full_ref, qkv_ref = refs
    blocks = len(come_refs)
    length = blocks * residues
    me = lax.axis_index("seq")
    for offset, come_ref in enumerate(come_refs):
        at = pl.multiple_of((me ^ offset) * residues, residues)
        for kind in range(3):
            qkv_ref[kind, pl.ds(at, residues), :] = come_ref[kind]
    others = bias_ref.shape[1]
    halves = LANES // columns
    rows = residues // halves

    @pl.when(pl.program_id(0) == 0)
    def _():
        pieces = jnp.concatenate(
            [bias_ref[:, other].reshape(blocks * rows, LANES) for other in range(others)], axis=1
        )
        for half in range(halves):
            place = where_matrix(
                (others * LANES, length),
                lambda r, l: ((r // columns) % halves == half)
                & ((r // LANES) * columns + r % columns == l),
            )
            placed = dot(pieces, place) * math.log2(math.e)
            for block in range(blocks):
                at = block * residues + half * rows
                full_ref[at : at + rows, :] = placed[block * rows : (block + 1) * rows]

    pack = LANES // head
    keys = qkv_ref[1]
    values = qkv_ref[2]
    lane = lax.broadcasted_iota(jnp.int32, (length, LANES), 1) // head
    zeros = jnp.zeros_like(keys)
    ones = jnp.ones_like(keys)
    key_of = [jnp.where(lane == place, keys, zeros) for place in range(pack)]
    value_of = [
        jnp.concatenate(
            [jnp.where(lane == place, values, zeros), jnp.where(lane == place, ones, zeros)], axis=1
        )
        for place in range(pack)
    ]
    value_all = jnp.concatenate(value_of, axis=0)
    per = row_step // residues
    for step in range(length // row_step):
        rows = slice(step * row_step, (step + 1) * row_step)
        queries = qkv_ref[0, rows, :]
        bias = full_ref[rows, :]
        weights = []
        for place in range(pack):
            scores = dot(queries, key_of[place], ((1,), (1,))) + bias + mask_ref[0, place : place + 1]
            weights.append(jnp.exp2(scores - jnp.max(scores, -1, keepdims=True)).astype(BF16))
        both = dot(jnp.concatenate(weights, axis=1), value_all)
        out_ref[step * per : (step + 1) * per] = (
            (both[:, :LANES] / both[:, LANES:]).astype(BF16).reshape(per, residues, LANES)
        )


def finish_kernel(
    sizes, mixed_ref, gate_ref, x_ref, wide_ref, gain_ref, up_ref, down_ref, out_ref
):
    residues, heads, head, _, groups = sizes
    pack = LANES // head
    gated = []
    for group in range(groups):
        lanes = slice(group * LANES, (group + 1) * LANES)
        gated.append(
            jnp.concatenate(
                [
                    (mixed_ref[h, :, lanes].astype(F32) * gate_ref[h, :, lanes]).astype(BF16)
                    for h in range(heads)
                ],
                axis=1,
            )
        )
    gated = jnp.concatenate(gated, axis=0)
    lane = lax.broadcasted_iota(jnp.int32, gated.shape, 1)
    place_of = (lane % LANES) // head
    chosen = jnp.concatenate(
        [jnp.where(place_of == place, gated, jnp.zeros_like(gated)) for place in range(pack)], axis=0
    )
    added = dot(chosen, wide_ref[...])
    order = [group * pack + place for place in range(pack) for group in range(groups)]
    x = jnp.concatenate([x_ref[seq] for seq in order], axis=0).astype(F32)
    after = x + added
    norm = normalized(after, gain_ref[...]).astype(BF16)
    hidden = jnp.maximum(dot(norm, up_ref[...]), 0.0).astype(BF16)
    result = after + dot(hidden, down_ref[...])
    for at, seq in enumerate(order):
        out_ref[seq] = result[at * residues : (at + 1) * residues]


def on_device(
    alignment,
    alignment_mask,
    residue_mask,
    pair_input,
    outer_gain,
    left_weight,
    right_weight,
    outer_weight,
    pair_gain,
    bias_weight,
    row_gain,
    query_weight,
    key_weight,
    value_weight,
    gate_weight,
    output_weight,
    transition_gain,
    up_weight,
    down_weight,
):
    seqs, residues, channels = alignment.shape
    columns, pair_width = pair_input.shape[1:]
    seq_axis, res_axis = lax.axis_size("seq"), lax.axis_size("res")
    heads = bias_weight.shape[1]
    head = query_weight.shape[1] // heads
    width = left_weight.shape[1]
    all_seqs, length = seqs * res_axis, residues * seq_axis
    shares = seq_axis // heads
    own = seqs // shares
    pack = LANES // head
    assert shares * heads == seq_axis and own % pack == 0
    blocks = seq_axis // res_axis
    assert blocks * residues == columns

    flat = alignment.reshape(seqs * residues, channels)
    wide = residues * width + LANES

    left, right = pl.pallas_call(
        functools.partial(factor_kernel, (seqs, residues, width)),
        out_shape=(jax.ShapeDtypeStruct((seqs, wide), BF16),) * 2,
        scratch_shapes=[
            pltpu.VMEM((channels // LANES, seqs * residues, LANES), F32),
            pltpu.VMEM((seqs * residues, channels), BF16),
        ],
        compiler_params=params(ALL_VMEM_BYTES),
        cost_estimate=pl.CostEstimate(
            flops=2 * seqs * residues * channels * 2 * PACK * width, bytes_accessed=1 << 20,
            transcendentals=0,
        ),
        name="factors",
    )(flat, alignment_mask, residue_mask[None], outer_gain[None], left_weight.T, right_weight.T)

    half = seq_axis // 2
    come = lax.ppermute(right, "seq", [(i, i ^ half) for i in range(seq_axis)])
    right_parts = swapped([right] * half, "seq")
    right_parts = right_parts + swapped([come] * half, "seq")

    left_all = swapped([left] * res_axis, "res")

    head_sizes = (seqs, residues, heads, head, shares)
    qkv = pl.pallas_call(
        functools.partial(project_kernel, head_sizes, head ** (-0.5) * math.log2(math.e)),
        out_shape=(jax.ShapeDtypeStruct((3, residues, own * head), BF16),) * seq_axis,
        scratch_shapes=[
            pltpu.VMEM((seqs * residues, channels), BF16),
            pltpu.VMEM((seq_axis, 3, residues, own * head), BF16),
        ],
        compiler_params=params(ALL_VMEM_BYTES),
        cost_estimate=pl.CostEstimate(
            flops=2 * seqs * residues * channels * 3 * heads * LANES, bytes_accessed=2 << 20,
            transcendentals=0,
        ),
        name="projections",
    )(flat, row_gain[None], query_weight, key_weight, value_weight)
    gates = pl.pallas_call(
        functools.partial(gate_kernel, head_sizes),
        out_shape=jax.ShapeDtypeStruct((seq_axis, residues, own * head), F32),
        scratch_shapes=[pltpu.VMEM((seqs * residues, channels), BF16)],
        compiler_params=params(ALL_VMEM_BYTES),
        cost_estimate=pl.CostEstimate(
            flops=2 * seqs * residues * channels * heads * LANES, bytes_accessed=2 << 20,
            transcendentals=seqs * residues * channels,
        ),
        name="gates",
    )(flat, row_gain[None], gate_weight)

    right_rows = pl.pallas_call(
        assemble_kernel,
        out_shape=jax.ShapeDtypeStruct((seq_axis, seqs, wide), BF16),
        compiler_params=params(),
        cost_estimate=pl.CostEstimate(flops=1 << 26, bytes_accessed=1 << 20, transcendentals=0),
        name="assemble",
    )(*right_parts)

    right_all = lax.all_to_all(right_rows, "res", split_axis=0, concat_axis=0, tiled=True)
    qkv_all = swapped(qkv, "seq")

    mask = pl.pallas_call(
        functools.partial(mask_kernel, (residues, shares)),
        grid=(1,),
        in_specs=[
            pl.BlockSpec((seq_axis, seqs, LANES), lambda _: (0, 0, residues * width // LANES))
        ],
        out_specs=whole((own // pack, pack, length)),
        out_shape=jax.ShapeDtypeStruct((own // pack, pack, length), F32),
        compiler_params=params(),
        cost_estimate=pl.CostEstimate(flops=1 << 26, bytes_accessed=1 << 17, transcendentals=0),
        name="mask",
    )(right_rows)

    quad = LANES // width
    wide_output = pl.pallas_call(
        functools.partial(widen_kernel, (heads, head)),
        out_shape=jax.ShapeDtypeStruct((heads * LANES, channels), BF16),
        compiler_params=params(ALL_VMEM_BYTES),
        cost_estimate=pl.CostEstimate(flops=1 << 28, bytes_accessed=1 << 19, transcendentals=0),
        name="widen",
    )(output_weight)
    halves = LANES // columns
    bias_rows = residues // halves
    pair_output, bias = pl.pallas_call(
        functools.partial(
            outer_kernel, (residues, columns, width, pair_width, all_seqs, shares)
        ),
        in_specs=[
            pl.BlockSpec(memory_space=pl.ANY if at == 1 else pltpu.VMEM)
            for at in range(5 + res_axis)
        ],
        out_shape=(
            jax.ShapeDtypeStruct(pair_input.shape, F32),
            jax.ShapeDtypeStruct((seq_axis, res_axis, bias_rows, LANES), BF16),
        ),
        scratch_shapes=[
            pltpu.VMEM((all_seqs, wide), BF16),
            pltpu.VMEM((residues // quad * columns, width * LANES), BF16),
            pltpu.VMEM((residues, columns, pair_width), BF16),
            pltpu.VMEM((heads, bias_rows, LANES), F32),
            pltpu.VMEM((width * LANES, quad * pair_width), BF16),
            pltpu.VMEM(outer_weight.shape, F32),
            pltpu.VMEM(pair_input.shape, F32),
            pltpu.SemaphoreType.DMA,
        ],
        compiler_params=params(ALL_VMEM_BYTES),
        cost_estimate=pl.CostEstimate(
            flops=2 * residues * columns * width * width * (all_seqs + 4 * pair_width),
            bytes_accessed=4 << 20,
            transcendentals=0,
        ),
        name="outer",
    )(
        right_all.reshape(res_axis, blocks, seqs, wide),
        pair_input,
        outer_weight,
        pair_gain[None],
        bias_weight.T,
        *left_all,
    )
    bias_all = lax.all_to_all(
        bias.reshape(seq_axis * res_axis, bias_rows, LANES),
        ("seq", "res"),
        split_axis=0,
        concat_axis=0,
        tiled=True,
    ).reshape(seq_axis, res_axis, bias_rows, LANES)

    mixed = pl.pallas_call(
        functools.partial(
            attention_kernel, (residues, columns, head, max(residues, min(length, ROW_STEP)))
        ),
        grid=(own // pack,),
        in_specs=[
            whole((seq_axis, res_axis, bias_rows, LANES)),
            pl.BlockSpec((1, pack, length), lambda g: (g, 0, 0)),
            *(pl.BlockSpec((3, residues, LANES), lambda g: (0, 0, g)),) * seq_axis,
        ],
        out_specs=pl.BlockSpec((seq_axis, residues, LANES), lambda g: (0, 0, g)),
        out_shape=jax.ShapeDtypeStruct((seq_axis, residues, own * head), BF16),
        scratch_shapes=[
            pltpu.VMEM((length, length), F32),
            pltpu.VMEM((3, length, LANES), BF16),
        ],
        compiler_params=params(),
        cost_estimate=pl.CostEstimate(
            flops=4 * own * length * length * LANES, bytes_accessed=2 << 20,
            transcendentals=own * length * length,
        ),
        name="attention",
    )(bias_all, mask, *qkv_all)

    mixed_home = lax.all_to_all(mixed, "seq", split_axis=0, concat_axis=0, tiled=True)

    steps = 2 * shares
    groups = seqs // pack // steps
    per_share = own // pack // groups
    if shares > 1:
        mixed_home = mixed_home.reshape(heads, shares, residues, own * head)
        gates = gates.reshape(heads, shares, residues, own * head)
        share_spec = pl.BlockSpec(
            (heads, None, residues, groups * LANES), lambda g: (0, g // per_share, 0, g % per_share)
        )
    else:
        share_spec = pl.BlockSpec((heads, residues, groups * LANES), lambda g: (0, 0, g))
    hidden = up_weight.shape[1]
    alignment_output = pl.pallas_call(
        functools.partial(finish_kernel, (residues, heads, head, shares, groups)),
        grid=(steps,),
        in_specs=[
            share_spec,
            share_spec,
            pl.BlockSpec((groups * pack, residues, channels), lambda g: (g, 0, 0)),
            whole((heads * LANES, channels)),
            whole((1, channels)),
            whole(up_weight.shape),
            whole(down_weight.shape),
        ],
        out_specs=pl.BlockSpec((groups * pack, residues, channels), lambda g: (g, 0, 0)),
        out_shape=jax.ShapeDtypeStruct(alignment.shape, F32),
        compiler_params=params(),
        cost_estimate=pl.CostEstimate(
            flops=2 * seqs * residues * channels * (4 * channels + 2 * hidden),
            bytes_accessed=4 << 20,
            transcendentals=0,
        ),
        name="finish",
    )(mixed_home, gates, alignment, wide_output, transition_gain[None], up_weight, down_weight)
    return (pair_output, alignment_output)


def solution(mesh):
    spread = P("res", "seq", None)
    pair = P("seq", "res", None)
    in_specs = (spread, P("res", "seq"), P(), pair) + (P(),) * 15

    return jax.shard_map(
        on_device, mesh=mesh, in_specs=in_specs, out_specs=(pair, spread), check_vma=False
    )
```

```python
import functools
import math

import jax
import jax.numpy as jnp
from jax import lax
from jax.experimental import pallas as pl
from jax.experimental.pallas import tpu as pltpu
from jax.sharding import PartitionSpec as P


EPSILON = 1e-05
MASKED = -1000000000.0
LANES = 128
ROW_STEP = 256
TOGETHER = 8
PACK = 8
VMEM_BYTES = 40 * 1024 * 1024
ALL_VMEM_BYTES = 60 * 1024 * 1024
F32 = jnp.float32
BF16 = jnp.bfloat16


def normalized(values, gain):
    center = values - jnp.mean(values, -1, keepdims=True)
    spread = jnp.mean(center * center, -1, keepdims=True)
    return center * lax.rsqrt(spread + EPSILON) * gain


def dot(left, right, dims=((1,), (0,))):
    return lax.dot_general(left, right, (dims, ((), ())), preferred_element_type=F32)


def where_matrix(shape, test):
    rows = lax.broadcasted_iota(jnp.int32, shape, 0)
    lanes = lax.broadcasted_iota(jnp.int32, shape, 1)
    return jnp.where(test(rows, lanes), 1.0, 0.0).astype(BF16)


def swapped(arrays, axis):
    size = lax.axis_size(axis)
    assert len(arrays) & (len(arrays) - 1) == 0 and size % len(arrays) == 0
    come = []
    for k, array in enumerate(arrays):
        pairs = [(i, i ^ k) for i in range(size)]
        come.append(lax.ppermute(array, axis, pairs) if k else array)
    return come


def whole(shape):
    return pl.BlockSpec(shape, lambda *_: (0,) * len(shape))


def params(limit=VMEM_BYTES):
    return pltpu.CompilerParams(vmem_limit_bytes=limit)


def factor_kernel(
    sizes,
    x_ref,
    mask_ref,
    residue_ref,
    gain_ref,
    left_w_ref,
    right_w_ref,
    left_ref,
    right_ref,
    norm_ref,
    rows_ref,
):
    seqs, residues, width = sizes
    norm = normalized(x_ref[...].astype(F32), gain_ref[...])
    groups = residues // PACK
    for part in range(norm_ref.shape[0]):
        lanes = slice(part * LANES, (part + 1) * LANES)
        norm_ref[part] = norm[:, lanes]
        for place in range(PACK):
            for group in range(groups):
                at = (place * groups + group) * seqs
                rows_ref[at : at + seqs, lanes] = norm_ref[
                    part, pl.ds(group * PACK + place, seqs, stride=residues), :
                ].astype(BF16)
    span = PACK * width
    spread_left = where_matrix((width, span), lambda r, l: r == l % width)
    spread_right = where_matrix((width, span), lambda r, l: r == l // PACK)
    left_wide = dot(left_w_ref[...], spread_left, ((0,), (0,))).astype(BF16)
    right_wide = dot(right_w_ref[...], spread_right, ((0,), (0,))).astype(BF16)
    rows = rows_ref[...]
    start = lax.axis_index("seq") * residues
    own = where_matrix((residue_ref.shape[1], residues), lambda r, l: r == l + start)
    row_live = dot(residue_ref[...].astype(F32).astype(BF16), own)
    live = (mask_ref[...].astype(F32) * row_live).astype(BF16)
    total = residues * width
    live_left = dot(live, where_matrix((residues, total), lambda r, l: r == l // width))
    live_right = dot(
        live,
        where_matrix((residues, total), lambda r, l: r == (l // span) * PACK + l % PACK),
    )
    live_plain = dot(live, where_matrix((residues, LANES), lambda r, l: r == l)).astype(BF16)
    lane = lax.broadcasted_iota(jnp.int32, (groups * seqs, span), 1)
    for wide, out_ref, live_wide, place_of in (
        (left_wide, left_ref, live_left, lane // width),
        (right_wide, right_ref, live_right, lane % PACK),
    ):
        product = dot(rows, wide)
        packed = product[: groups * seqs]
        for place in range(1, PACK):
            packed = jnp.where(
                place_of == place,
                product[place * groups * seqs : (place + 1) * groups * seqs],
                packed,
            )
        pieces = []
        for group in range(groups):
            piece = packed[group * seqs : (group + 1) * seqs]
            pieces.append((piece * live_wide[:, group * span : (group + 1) * span]).astype(BF16))
        for group in range(groups):
            out_ref[:, group * span : (group + 1) * span] = pieces[group]
        out_ref[:, total:] = live_plain


def project_heads(sizes, x_ref, gain_ref, rows_ref, w_refs, write):
    seqs, residues, heads, head, shares = sizes
    pack = LANES // head
    groups = seqs // pack
    block = groups * residues
    norm = normalized(x_ref[...].astype(F32), gain_ref[...]).astype(BF16)
    for seq in range(seqs):
        at = (seq % pack) * block + (seq // pack) * residues
        rows_ref[at : at + residues, :] = norm[seq * residues : (seq + 1) * residues]
    pair = 2 * LANES
    place_of = (lax.broadcasted_iota(jnp.int32, (block, pair), 1) % LANES) // head
    own = groups // shares
    for kind, w_ref in enumerate(w_refs):
        for two in range(heads // 2):
            base = two * 2 * head
            spread = where_matrix(
                (heads * head, pair), lambda r, l: r == base + (l // LANES) * head + l % head
            )
            product = dot(rows_ref[...], dot(w_ref[...], spread).astype(BF16))
            packed = product[:block]
            for place in range(1, pack):
                packed = jnp.where(
                    place_of == place, product[place * block : (place + 1) * block], packed
                )
            for one in range(2):
                done = packed[:, one * LANES : (one + 1) * LANES]
                for group in range(groups):
                    to = (two * 2 + one) * shares + group // own
                    lanes = slice((group % own) * LANES, (group % own + 1) * LANES)
                    write(kind, to, lanes, done[group * residues : (group + 1) * residues])


def gate_kernel(sizes, x_ref, gain_ref, w_ref, gate_ref, rows_ref):
    def write(kind, to, lanes, piece):
        gate_ref[to, :, lanes] = jax.nn.sigmoid(piece)

    project_heads(sizes, x_ref, gain_ref, rows_ref, [w_ref], write)


def project_kernel(sizes, scale, x_ref, gain_ref, qw_ref, kw_ref, vw_ref, *refs):
    *sent_refs, rows_ref, qkv_ref = refs

    def write(kind, to, lanes, piece):
        qkv_ref[to, kind, :, lanes] = (piece * scale if kind == 0 else piece).astype(BF16)

    project_heads(sizes, x_ref, gain_ref, rows_ref, [qw_ref, kw_ref, vw_ref], write)
    me = lax.axis_index("seq")
    for offset, sent_ref in enumerate(sent_refs):
        sent_ref[...] = qkv_ref[me ^ offset]


def assemble_kernel(*refs):
    *part_refs, out_ref = refs
    me = lax.axis_index("seq")
    for offset, part_ref in enumerate(part_refs):
        out_ref[me ^ offset] = part_ref[...]


def mask_kernel(sizes, rows_ref, out_ref):
    residues, shares = sizes
    blocks, seqs, _ = rows_ref.shape
    groups, pack, length = out_ref.shape
    live = jnp.zeros((seqs, length), F32)
    for block in range(blocks):
        place = where_matrix((LANES, length), lambda r, l: l == r + block * residues)
        inside = lax.broadcasted_iota(jnp.int32, (LANES, length), 0) < residues
        live = live + dot(rows_ref[block], jnp.where(inside, place, jnp.zeros_like(place)))
    if shares > 1:
        first = (lax.axis_index("seq") % shares) * groups * pack
        chosen = where_matrix((groups * pack, seqs), lambda r, l: l == r + first)
        live = dot(chosen, live.astype(BF16))
    added = (1.0 - live) * MASKED
    for group in range(groups):
        out_ref[group] = added[group * pack : (group + 1) * pack]


def widen_kernel(sizes, out_w_ref, gain_ref, wide_ref, gain_out_ref):
    heads, head = sizes
    gain_out_ref[...] = gain_ref[...]
    spread = where_matrix(
        (heads * LANES, heads * head), lambda r, l: (r // LANES) * head + r % head == l
    )
    wide_ref[...] = dot(spread, out_w_ref[...]).astype(BF16)


def outer_kernel(sizes, right_ref, pair_ref, weight_ref, gain_ref, bias_w_ref, *refs):
    residues, columns, width, pair_width, seqs, shares = sizes
    members = right_ref.shape[0]
    left_refs = refs[:members]
    out_ref, bias_ref, left_ref, stage_ref, norm_ref, bias_rows_ref = refs[members : members + 6]
    held_ref, plain_ref, held_pair_ref, pair_sem = refs[members + 6 :]
    pair_copy = pltpu.make_async_copy(pair_ref, held_pair_ref, pair_sem)
    pair_copy.start()
    quad = LANES // width
    plain_ref[...] = weight_ref[...].astype(F32)
    held_ref[...] = jnp.zeros_like(held_ref)
    for e in range(width):
        piece = plain_ref[pl.ds(e, width, stride=width), :].astype(BF16)
        for place in range(quad):
            row = e * LANES + place * width
            held_ref[row : row + width, place * pair_width : (place + 1) * pair_width] = piece
    share = seqs // members
    me = lax.axis_index("res")
    for offset, member_ref in enumerate(left_refs):
        at = pl.multiple_of((me ^ offset) * share, share)
        left_ref[pl.ds(at, share), :] = member_ref[...]
    span = PACK * width
    groups = residues // quad
    total = residues * width
    blocks = right_ref.shape[1]
    live_left = left_ref[:, total : total + LANES]
    counts = []
    for block in range(blocks):
        live_right = right_ref[:, block, :, total : total + LANES].reshape(seqs, LANES)
        counts.append(dot(live_right.T, live_left)[:residues])
        for two in range(residues // (2 * PACK)):
            flipped = []
            for one in range(2):
                lanes = slice((two * 2 + one) * span, (two * 2 + one + 1) * span)
                flipped.append(right_ref[:, block, :, lanes].reshape(seqs, span).T)
            row = block * residues + two * 2 * PACK
            for chunk in range(total // (2 * LANES)):
                left = left_ref[:, chunk * 2 * LANES : (chunk + 1) * 2 * LANES]
                products = [
                    dot(member, left).reshape(width, PACK, 2 * LANES) for member in flipped
                ]
                joined = jnp.concatenate(products, axis=1).astype(BF16)
                for one in range(2):
                    at = (chunk * 2 + one) * columns + row
                    for e in range(width):
                        stage_ref[at : at + 2 * PACK, e * LANES : (e + 1) * LANES] = joined[
                            e, :, one * LANES : (one + 1) * LANES
                        ]
    scale = 1.0 / jnp.maximum(jnp.concatenate(counts, axis=0), 1.0)
    gain = gain_ref[...]
    pair_copy.wait()
    for two in range(quad // 2):
        lanes = slice(two * 2 * pair_width, (two + 1) * 2 * pair_width)
        update = dot(stage_ref[...], held_ref[:, lanes])
        for group in range(groups):
            for one in range(2):
                i = group * quad + two * 2 + one
                piece = update[
                    group * columns : (group + 1) * columns,
                    one * pair_width : (one + 1) * pair_width,
                ]
                value = held_pair_ref[i] + piece * scale[:, i : i + 1]
                out_ref[i] = value
                norm_ref[i] = normalized(value, gain).astype(BF16)
    halves = LANES // columns
    rows = residues // halves
    for row in range(rows):
        joined = jnp.concatenate([norm_ref[row + half * rows] for half in range(halves)], axis=0)
        bias = dot(bias_w_ref[...], joined, ((1,), (1,)))
        for head in range(bias_w_ref.shape[0]):
            bias_rows_ref[head, row : row + 1, :] = bias[head : head + 1, :]
    for to in range(bias_ref.shape[0]):
        piece = bias_rows_ref[to // shares].astype(BF16)
        for other in range(bias_ref.shape[1]):
            bias_ref[to, other] = piece


def attention_kernel(sizes, bias_ref, mask_ref, *refs):
    residues, columns, head, row_step = sizes
    *come_refs, out_ref, full_ref, qkv_ref = refs
    blocks = len(come_refs)
    length = blocks * residues
    me = lax.axis_index("seq")
    for offset, come_ref in enumerate(come_refs):
        at = pl.multiple_of((me ^ offset) * residues, residues)
        for kind in range(3):
            qkv_ref[kind, pl.ds(at, residues), :] = come_ref[kind]
    others = bias_ref.shape[1]
    halves = LANES // columns
    rows = residues // halves

    @pl.when(pl.program_id(0) == 0)
    def _():
        pieces = jnp.concatenate(
            [bias_ref[:, other].reshape(blocks * rows, LANES) for other in range(others)], axis=1
        )
        for half in range(halves):
            place = where_matrix(
                (others * LANES, length),
                lambda r, l: ((r // columns) % halves == half)
                & ((r // LANES) * columns + r % columns == l),
            )
            placed = dot(pieces, place) * math.log2(math.e)
            for block in range(blocks):
                at = block * residues + half * rows
                full_ref[at : at + rows, :] = placed[block * rows : (block + 1) * rows]

    pack = LANES // head
    lane = lax.broadcasted_iota(jnp.int32, (length, LANES), 1) // head
    per = row_step // residues
    for group in range(out_ref.shape[2] // LANES):
        lanes = slice(group * LANES, (group + 1) * LANES)
        keys = qkv_ref[1, :, lanes]
        values = qkv_ref[2, :, lanes]
        zeros = jnp.zeros_like(keys)
        ones = jnp.ones_like(keys)
        key_of = [jnp.where(lane == place, keys, zeros) for place in range(pack)]
        value_of = [
            jnp.concatenate(
                [jnp.where(lane == place, member, zeros) for member in (values, ones)], axis=1
            )
            for place in range(pack)
        ]
        value_all = jnp.concatenate(value_of, axis=0)
        for step in range(length // row_step):
            rows = slice(step * row_step, (step + 1) * row_step)
            queries = qkv_ref[0, rows, lanes]
            bias = full_ref[rows, :]
            weights = []
            for place in range(pack):
                scores = dot(queries, key_of[place], ((1,), (1,))) + bias
                scores = scores + mask_ref[group, place : place + 1]
                weights.append(
                    jnp.exp2(scores - jnp.max(scores, -1, keepdims=True)).astype(BF16)
                )
            both = dot(jnp.concatenate(weights, axis=1), value_all)
            out_ref[step * per : (step + 1) * per, :, lanes] = (
                (both[:, :LANES] / both[:, LANES:]).astype(BF16).reshape(per, residues, LANES)
            )


def finish_kernel(
    sizes, mixed_ref, gate_ref, x_ref, wide_ref, gain_ref, up_ref, down_ref, out_ref
):
    residues, heads, head, _, groups = sizes
    pack = LANES // head
    gated = []
    for group in range(groups):
        lanes = slice(group * LANES, (group + 1) * LANES)
        gated.append(
            jnp.concatenate(
                [
                    (mixed_ref[h, :, lanes].astype(F32) * gate_ref[h, :, lanes]).astype(BF16)
                    for h in range(heads)
                ],
                axis=1,
            )
        )
    gated = jnp.concatenate(gated, axis=0)
    lane = lax.broadcasted_iota(jnp.int32, gated.shape, 1)
    place_of = (lane % LANES) // head
    chosen = jnp.concatenate(
        [jnp.where(place_of == place, gated, jnp.zeros_like(gated)) for place in range(pack)], axis=0
    )
    added = dot(chosen, wide_ref[...])
    order = [group * pack + place for place in range(pack) for group in range(groups)]
    x = jnp.concatenate([x_ref[seq] for seq in order], axis=0).astype(F32)
    after = x + added
    norm = normalized(after, gain_ref[...]).astype(BF16)
    hidden = jnp.maximum(dot(norm, up_ref[...]), 0.0).astype(BF16)
    result = after + dot(hidden, down_ref[...])
    for at, seq in enumerate(order):
        out_ref[seq] = result[at * residues : (at + 1) * residues]


def on_device(
    alignment,
    alignment_mask,
    residue_mask,
    pair_input,
    outer_gain,
    left_weight,
    right_weight,
    outer_weight,
    pair_gain,
    bias_weight,
    row_gain,
    query_weight,
    key_weight,
    value_weight,
    gate_weight,
    output_weight,
    transition_gain,
    up_weight,
    down_weight,
):
    seqs, residues, channels = alignment.shape
    columns, pair_width = pair_input.shape[1:]
    seq_axis, res_axis = lax.axis_size("seq"), lax.axis_size("res")
    heads = bias_weight.shape[1]
    head = query_weight.shape[1] // heads
    width = left_weight.shape[1]
    all_seqs, length = seqs * res_axis, residues * seq_axis
    shares = seq_axis // heads
    own = seqs // shares
    pack = LANES // head
    assert shares * heads == seq_axis and own % pack == 0
    blocks = seq_axis // res_axis
    assert blocks * residues == columns

    flat = alignment.reshape(seqs * residues, channels)
    wide = residues * width + LANES

    left, right = pl.pallas_call(
        functools.partial(factor_kernel, (seqs, residues, width)),
        out_shape=(jax.ShapeDtypeStruct((seqs, wide), BF16),) * 2,
        scratch_shapes=[
            pltpu.VMEM((channels // LANES, seqs * residues, LANES), F32),
            pltpu.VMEM((seqs * residues, channels), BF16),
        ],
        compiler_params=params(ALL_VMEM_BYTES),
        cost_estimate=pl.CostEstimate(
            flops=2 * seqs * residues * channels * 2 * PACK * width, bytes_accessed=1 << 20,
            transcendentals=0,
        ),
        name="factors",
    )(flat, alignment_mask, residue_mask[None], outer_gain[None], left_weight.T, right_weight.T)

    half = seq_axis // 2
    come = lax.ppermute(right, "seq", [(i, i ^ half) for i in range(seq_axis)])
    right_parts = swapped([right] * half, "seq")
    right_parts = right_parts + swapped([come] * half, "seq")

    left_all = swapped([left] * res_axis, "res")

    head_sizes = (seqs, residues, heads, head, shares)
    qkv = pl.pallas_call(
        functools.partial(project_kernel, head_sizes, head ** (-0.5) * math.log2(math.e)),
        out_shape=(jax.ShapeDtypeStruct((3, residues, own * head), BF16),) * seq_axis,
        scratch_shapes=[
            pltpu.VMEM((seqs * residues, channels), BF16),
            pltpu.VMEM((seq_axis, 3, residues, own * head), BF16),
        ],
        compiler_params=params(ALL_VMEM_BYTES),
        cost_estimate=pl.CostEstimate(
            flops=2 * seqs * residues * channels * 3 * heads * LANES, bytes_accessed=2 << 20,
            transcendentals=0,
        ),
        name="projections",
    )(flat, row_gain[None], query_weight, key_weight, value_weight)
    gates = pl.pallas_call(
        functools.partial(gate_kernel, head_sizes),
        out_shape=jax.ShapeDtypeStruct((seq_axis, residues, own * head), F32),
        scratch_shapes=[pltpu.VMEM((seqs * residues, channels), BF16)],
        compiler_params=params(ALL_VMEM_BYTES),
        cost_estimate=pl.CostEstimate(
            flops=2 * seqs * residues * channels * heads * LANES, bytes_accessed=2 << 20,
            transcendentals=seqs * residues * channels,
        ),
        name="gates",
    )(flat, row_gain[None], gate_weight)

    right_rows = pl.pallas_call(
        assemble_kernel,
        out_shape=jax.ShapeDtypeStruct((seq_axis, seqs, wide), BF16),
        compiler_params=params(),
        cost_estimate=pl.CostEstimate(flops=1 << 26, bytes_accessed=1 << 20, transcendentals=0),
        name="assemble",
    )(*right_parts)

    right_all = lax.all_to_all(right_rows, "res", split_axis=0, concat_axis=0, tiled=True)
    qkv_all = swapped(qkv, "seq")

    mask = pl.pallas_call(
        functools.partial(mask_kernel, (residues, shares)),
        grid=(1,),
        in_specs=[
            pl.BlockSpec((seq_axis, seqs, LANES), lambda _: (0, 0, residues * width // LANES))
        ],
        out_specs=whole((own // pack, pack, length)),
        out_shape=jax.ShapeDtypeStruct((own // pack, pack, length), F32),
        compiler_params=params(),
        cost_estimate=pl.CostEstimate(flops=1 << 26, bytes_accessed=1 << 17, transcendentals=0),
        name="mask",
    )(right_rows)

    quad = LANES // width
    wide_output, last_gain = pl.pallas_call(
        functools.partial(widen_kernel, (heads, head)),
        out_shape=(
            jax.ShapeDtypeStruct((heads * LANES, channels), BF16),
            jax.ShapeDtypeStruct((1, channels), F32),
        ),
        compiler_params=params(),
        cost_estimate=pl.CostEstimate(flops=1 << 28, bytes_accessed=1 << 19, transcendentals=0),
        name="widen",
    )(output_weight, transition_gain[None])
    halves = LANES // columns
    bias_rows = residues // halves
    pair_output, bias = pl.pallas_call(
        functools.partial(
            outer_kernel, (residues, columns, width, pair_width, all_seqs, shares)
        ),
        in_specs=[
            pl.BlockSpec(memory_space=pl.ANY if at == 1 else pltpu.VMEM)
            for at in range(5 + res_axis)
        ],
        out_shape=(
            jax.ShapeDtypeStruct(pair_input.shape, F32),
            jax.ShapeDtypeStruct((seq_axis, res_axis, bias_rows, LANES), BF16),
        ),
        scratch_shapes=[
            pltpu.VMEM((all_seqs, wide), BF16),
            pltpu.VMEM((residues // quad * columns, width * LANES), BF16),
            pltpu.VMEM((residues, columns, pair_width), BF16),
            pltpu.VMEM((heads, bias_rows, LANES), F32),
            pltpu.VMEM((width * LANES, quad * pair_width), BF16),
            pltpu.VMEM(outer_weight.shape, F32),
            pltpu.VMEM(pair_input.shape, F32),
            pltpu.SemaphoreType.DMA,
        ],
        compiler_params=params(),
        cost_estimate=pl.CostEstimate(
            flops=2 * residues * columns * width * width * (all_seqs + 4 * pair_width),
            bytes_accessed=4 << 20,
            transcendentals=0,
        ),
        name="outer",
    )(
        right_all.reshape(res_axis, blocks, seqs, wide),
        pair_input,
        outer_weight,
        pair_gain[None],
        bias_weight.T,
        *left_all,
    )
    bias_all = lax.all_to_all(
        bias.reshape(seq_axis * res_axis, bias_rows, LANES),
        ("seq", "res"),
        split_axis=0,
        concat_axis=0,
        tiled=True,
    ).reshape(seq_axis, res_axis, bias_rows, LANES)

    together = math.gcd(own // pack, TOGETHER)
    mixed = pl.pallas_call(
        functools.partial(
            attention_kernel, (residues, columns, head, max(residues, min(length, ROW_STEP)))
        ),
        grid=(own // pack // together,),
        in_specs=[
            whole((seq_axis, res_axis, bias_rows, LANES)),
            pl.BlockSpec((together, pack, length), lambda g: (g, 0, 0)),
            *(pl.BlockSpec((3, residues, together * LANES), lambda g: (0, 0, g)),) * seq_axis,
        ],
        out_specs=pl.BlockSpec((seq_axis, residues, together * LANES), lambda g: (0, 0, g)),
        out_shape=jax.ShapeDtypeStruct((seq_axis, residues, own * head), BF16),
        scratch_shapes=[
            pltpu.VMEM((length, length), F32),
            pltpu.VMEM((3, length, together * LANES), BF16),
        ],
        compiler_params=params(),
        cost_estimate=pl.CostEstimate(
            flops=4 * own * length * length * LANES, bytes_accessed=2 << 20,
            transcendentals=own * length * length,
        ),
        name="attention",
    )(bias_all, mask, *qkv_all)

    mixed_home = lax.all_to_all(mixed, "seq", split_axis=0, concat_axis=0, tiled=True)

    steps = 2 * shares
    groups = seqs // pack // steps
    per_share = own // pack // groups
    if shares > 1:
        mixed_home = mixed_home.reshape(heads, shares, residues, own * head)
        gates = gates.reshape(heads, shares, residues, own * head)
        share_spec = pl.BlockSpec(
            (heads, None, residues, groups * LANES), lambda g: (0, g // per_share, 0, g % per_share)
        )
    else:
        share_spec = pl.BlockSpec((heads, residues, groups * LANES), lambda g: (0, 0, g))
    hidden = up_weight.shape[1]
    alignment_output = pl.pallas_call(
        functools.partial(finish_kernel, (residues, heads, head, shares, groups)),
        grid=(steps,),
        in_specs=[
            share_spec,
            share_spec,
            pl.BlockSpec((groups * pack, residues, channels), lambda g: (g, 0, 0)),
            whole((heads * LANES, channels)),
            whole((1, channels)),
            whole(up_weight.shape),
            whole(down_weight.shape),
        ],
        out_specs=pl.BlockSpec((groups * pack, residues, channels), lambda g: (g, 0, 0)),
        out_shape=jax.ShapeDtypeStruct(alignment.shape, F32),
        compiler_params=params(),
        cost_estimate=pl.CostEstimate(
            flops=2 * seqs * residues * channels * (4 * channels + 2 * hidden),
            bytes_accessed=4 << 20,
            transcendentals=0,
        ),
        name="finish",
    )(mixed_home, gates, alignment, wide_output, last_gain, up_weight, down_weight)
    return (pair_output, alignment_output)


def solution(mesh):
    spread = P("res", "seq", None)
    pair = P("seq", "res", None)
    in_specs = (spread, P("res", "seq"), P(), pair) + (P(),) * 15

    return jax.shard_map(
        on_device, mesh=mesh, in_specs=in_specs, out_specs=(pair, spread), check_vma=False
    )
```
